8 devices in a mesh: col: 2 (over z, y), row: 4 (over x, core).
Axes of the slice: x: 2, y: 2, z: 1, core: 2. Of those that a mesh axis runs over, the one named last changes fastest.
Arguments:
- x_in: bfloat16 [16384, 2048], P('row', 'col')
- ln_gain: float32 [2048], P('col')
- ln_bias: float32 [2048], P('col')
- w_up: bfloat16 [2048, 8192], P('row', 'col')
- b_up: bfloat16 [8192], P('col')
- w_down: bfloat16 [8192, 2048], P('row', 'col')
- b_down: bfloat16 [2048], P('col')
- dy_out: bfloat16 [16384, 2048], P('row', 'col')
Outputs:
- output 1: bfloat16 [16384, 2048], P('row', 'col')
- output 2: bfloat16 [16384, 2048], P('row', 'col')
- output 3: bfloat16 [2048, 8192], P('row', 'col')
- output 4: float32 [8192], P('col')
- output 5: bfloat16 [8192, 2048], P('row', 'col')
- output 6: float32 [2048], P('col')
- output 7: float32 [2048], P('col')
- output 8: float32 [2048], P('col')
All inputs are finite; a program needn't handle non-finite values.
Results may differ from the reference program's by a relative error of at most 0.0112855.
Values are sent between devices in bfloat16 or wider.
A program may use at most 1 GiB of HBM per device.

```python
import jax
import jax.numpy as jnp
from jax import lax

TOKENS = 16384
D = 2048
FF = 8192
LN_EPS = 1e-5
GELU_K = 0.7978845608028654
GELU_A = 0.044715


def setup_inputs(seed: int = 0) -> dict:
    keys = jax.random.split(jax.random.key(seed), 12)
    col_mean = jax.random.normal(keys[0], (1, D), jnp.float32)
    col_scale = 0.5 + jax.random.uniform(keys[1], (1, D), jnp.float32)
    row_shift = 0.5 * jax.random.normal(keys[2], (TOKENS, 1), jnp.float32)
    x_base = jax.random.normal(keys[3], (TOKENS, D), jnp.float32)
    x_in = (x_base * col_scale + col_mean + row_shift).astype(jnp.bfloat16)
    ln_gain = 0.5 + jax.random.uniform(keys[4], (D,), jnp.float32)
    ln_bias = 0.3 * jax.random.normal(keys[5], (D,), jnp.float32)
    w_up = (jax.random.normal(keys[6], (D, FF), jnp.float32) * D ** -0.5).astype(jnp.bfloat16)
    b_up = (0.5 * jax.random.normal(keys[7], (FF,), jnp.float32)).astype(jnp.bfloat16)
    w_down = (jax.random.normal(keys[8], (FF, D), jnp.float32) * (1.5 * FF ** -0.5)).astype(jnp.bfloat16)
    b_down = (0.5 * jax.random.normal(keys[9], (D,), jnp.float32)).astype(jnp.bfloat16)
    dy_out = jax.random.normal(keys[10], (TOKENS, D), jnp.float32).astype(jnp.bfloat16)
    return {'x_in': x_in, 'ln_gain': ln_gain, 'ln_bias': ln_bias, 'w_up': w_up, 'b_up': b_up, 'w_down': w_down, 'b_down': b_down, 'dy_out': dy_out}


def gelu_grad(u_val):
    tanh_val = jnp.tanh(GELU_K * (u_val + GELU_A * u_val * u_val * u_val))
    slope = GELU_K * (1.0 + 3.0 * GELU_A * u_val * u_val)
    return 0.5 * (1.0 + tanh_val) + 0.5 * u_val * (1.0 - tanh_val * tanh_val) * slope


def reference(x_in, ln_gain, ln_bias, w_up, b_up, w_down, b_down, dy_out):
    width = x_in.shape[1]
    x_f32 = x_in.astype(jnp.float32)
    mean_x = jnp.sum(x_f32, axis=1, keepdims=True) / width
    mean_sq = jnp.sum(x_f32 * x_f32, axis=1, keepdims=True) / width
    inv_std = lax.rsqrt(mean_sq - mean_x * mean_x + LN_EPS)
    x_hat = (x_f32 - mean_x) * inv_std
    z_act = (x_hat * ln_gain + ln_bias).astype(jnp.bfloat16)
    u_pre = (jnp.dot(z_act, w_up, preferred_element_type=jnp.float32) + b_up.astype(jnp.float32)).astype(jnp.bfloat16)
    u_f32 = u_pre.astype(jnp.float32)
    a_act = jax.nn.gelu(u_f32, approximate=True).astype(jnp.bfloat16)
    y_out = (x_f32 + jnp.dot(a_act, w_down, preferred_element_type=jnp.float32) + b_down.astype(jnp.float32)).astype(jnp.bfloat16)
    dy_f32 = dy_out.astype(jnp.float32)
    d_act = jnp.dot(dy_out, w_down.T, preferred_element_type=jnp.float32)
    du_pre = (d_act * gelu_grad(u_f32)).astype(jnp.bfloat16)
    dw_down = jnp.dot(a_act.T, dy_out, preferred_element_type=jnp.float32).astype(jnp.bfloat16)
    db_down = jnp.sum(dy_f32, axis=0)
    dw_up = jnp.dot(z_act.T, du_pre, preferred_element_type=jnp.float32).astype(jnp.bfloat16)
    db_up = jnp.sum(du_pre.astype(jnp.float32), axis=0)
    dz_act = jnp.dot(du_pre, w_up.T, preferred_element_type=jnp.float32)
    d_gain = jnp.sum(dz_act * x_hat, axis=0)
    d_bias = jnp.sum(dz_act, axis=0)
    d_xhat = dz_act * ln_gain
    mean_dxh = jnp.sum(d_xhat, axis=1, keepdims=True) / width
    mean_dxh_xh = jnp.sum(d_xhat * x_hat, axis=1, keepdims=True) / width
    dx_in = (dy_f32 + inv_std * (d_xhat - mean_dxh - x_hat * mean_dxh_xh)).astype(jnp.bfloat16)
    return (y_out, dx_in, dw_up, db_up, dw_down, db_down, d_gain, d_bias)
```

```python
import jax
import jax.numpy as jnp
from jax import lax
from jax.experimental import pallas as pl
from jax.experimental.pallas import tpu as pltpu
from jax.sharding import PartitionSpec as P


LN_EPS = 1e-5
GELU_K = 0.7978845608028654
GELU_A = 0.044715
CONTRACT_ROWS = (((0,), (0,)), ((), ()))
CONTRACT_COLS = (((1,), (1,)), ((), ()))
CONTRACT_MM = (((1,), (0,)), ((), ()))
NX = 4
NDY = 2
SUB = 256
VMEM = 58 * 1024 * 1024


def half_sigmoid(u_val, sq):
    return 0.5 + 0.5 * jnp.tanh(u_val * (GELU_K + (GELU_K * GELU_A) * sq))


def gelu_grad(u_val):
    sq = u_val * u_val
    half = half_sigmoid(u_val, sq)
    return half + (half * (1.0 - half) * u_val) * (2.0 * GELU_K + (6.0 * GELU_K * GELU_A) * sq)


def dot32(a, b, dims=CONTRACT_MM):
    return lax.dot_general(a, b, dims, preferred_element_type=jnp.float32)


def ln_kernel(c_ref, xl_ref, xr_ref, g_ref, b_ref, *refs):
    z_ref, st_ref = refs[-2:]
    width = xl_ref.shape[1]
    first = c_ref[0] == 0
    xl = xl_ref[...].astype(jnp.float32)
    xr = xr_ref[...].astype(jnp.float32)
    total = jnp.sum(xl, axis=1, keepdims=True) + jnp.sum(xr, axis=1, keepdims=True)
    square = jnp.sum(xl * xl, axis=1, keepdims=True) + jnp.sum(xr * xr, axis=1, keepdims=True)
    mean = total / (2 * width)
    inv = lax.rsqrt(square / (2 * width) - mean * mean + LN_EPS)
    hl = (xl - mean) * inv
    hr = (xr - mean) * inv
    lo = jnp.where(first, hl, hr)
    hi = jnp.where(first, hr, hl)
    z_ref[:, :width] = (lo * g_ref[:, :width] + b_ref[:, :width]).astype(z_ref.dtype)
    z_ref[:, width:] = (hi * g_ref[:, width:] + b_ref[:, width:]).astype(z_ref.dtype)
    lane = lax.broadcasted_iota(jnp.int32, st_ref.shape, 1)
    st_ref[...] = jnp.where(lane == 0, mean, inv)


def ln_call(cvec, x_in, x_rem, gain, bias, k, z_buf):
    rows, width = x_rem.shape
    tokens = x_in.shape[0]
    bm = 256
    off = k * rows // bm
    in_specs = [
        pl.BlockSpec((bm, width), lambda i, c: (off + i, 0)),
        pl.BlockSpec((bm, width), lambda i, c: (i, 0)),
        pl.BlockSpec((1, 2 * width), lambda i, c: (0, 0)),
        pl.BlockSpec((1, 2 * width), lambda i, c: (0, 0)),
    ]
    args = [cvec, x_in, x_rem, gain, bias]
    alias = {}
    if z_buf is not None:
        in_specs.append(pl.BlockSpec(memory_space=pl.ANY))
        args.append(z_buf)
        alias = {5: 0}
    return pl.pallas_call(
        ln_kernel,
        grid_spec=pltpu.PrefetchScalarGridSpec(
            num_scalar_prefetch=1,
            grid=(rows // bm,),
            in_specs=in_specs,
            out_specs=[
                pl.BlockSpec((bm, 2 * width), lambda i, c: (off + i, 0)),
                pl.BlockSpec((bm, 128), lambda i, c: (i, 0)),
            ],
        ),
        out_shape=[
            jax.ShapeDtypeStruct((tokens, 2 * width), jnp.bfloat16),
            jax.ShapeDtypeStruct((rows, 128), jnp.float32),
        ],
        input_output_aliases=alias,
        compiler_params=pltpu.CompilerParams(vmem_limit_bytes=VMEM),
        cost_estimate=pl.CostEstimate(flops=rows * width * 400, bytes_accessed=rows * width * 8, transcendentals=0),
    )(*args)


def ua_kernel(c_ref, z_ref, w_ref, b_ref, *refs):
    u_ref, a_ref = refs[-2:]
    for i in range(z_ref.shape[0] // SUB):
        part = pl.ds(i * SUB, SUB)
        u = (dot32(z_ref[part, :], w_ref[...]) + b_ref[...]).astype(u_ref.dtype)
        u_ref[part, :] = u
        u32 = u.astype(jnp.float32)
        a_ref[part, :] = (u32 * half_sigmoid(u32, u32 * u32)).astype(a_ref.dtype)


def ua_call(cvec, z_buf, w_half, b_half, k, other, bufs):
    tokens, width = z_buf.shape
    ffh = w_half.shape[1]
    rows = tokens // NX
    bn = 512
    nb = ffh // bn

    def col(j, c):
        return ((1 - c[0]) if other else c[0]) * nb + j

    in_specs = [
        pl.BlockSpec((rows, width), lambda j, c: (k, 0)),
        pl.BlockSpec((width, bn), lambda j, c: (0, j)),
        pl.BlockSpec((1, bn), lambda j, c: (0, j)),
    ]
    args = [cvec, z_buf, w_half, b_half]
    alias = {}
    if bufs is not None:
        in_specs += [pl.BlockSpec(memory_space=pl.ANY)] * 2
        args += list(bufs)
        alias = {4: 0, 5: 1}
    out = pl.BlockSpec((rows, bn), lambda j, c: (k, col(j, c)))
    shape = jax.ShapeDtypeStruct((tokens, 2 * ffh), jnp.bfloat16)
    return pl.pallas_call(
        ua_kernel,
        grid_spec=pltpu.PrefetchScalarGridSpec(
            num_scalar_prefetch=1, grid=(nb,), in_specs=in_specs, out_specs=[out, out]),
        out_shape=[shape, shape],
        input_output_aliases=alias,
        compiler_params=pltpu.CompilerParams(vmem_limit_bytes=VMEM),
        cost_estimate=pl.CostEstimate(
            flops=2 * rows * width * ffh, bytes_accessed=2 * (rows * width + width * ffh + 2 * rows * ffh),
            transcendentals=rows * ffh),
    )(*args)


def du_kernel(c_ref, yl_ref, yr_ref, wl_ref, wr_ref, u_ref, *refs):
    du_ref, sum_ref = refs[-2:]
    total = jnp.zeros(sum_ref.shape, jnp.float32)
    for i in range(yl_ref.shape[0] // SUB):
        part = pl.ds(i * SUB, SUB)
        da = dot32(yl_ref[part, :], wl_ref[...], CONTRACT_COLS) + dot32(yr_ref[part, :], wr_ref[...], CONTRACT_COLS)
        du = (da * gelu_grad(u_ref[part, :].astype(jnp.float32))).astype(du_ref.dtype)
        du_ref[part, :] = du
        total += jnp.sum(du.astype(jnp.float32).reshape(SUB // 8, 8, -1), axis=0)
    sum_ref[...] = total


def du_call(cvec, dy_out, dy_rem, w_own, w_oth, u_buf, k, other, buf):
    tokens, dloc = dy_out.shape
    rows = dy_rem.shape[0]
    ffh = w_own.shape[0] // 2
    bn = 512
    nb = ffh // bn

    def off(j, c):
        return ((1 - c[0]) if other else c[0]) * nb + j

    in_specs = [
        pl.BlockSpec((rows, dloc), lambda j, c: (k, 0)),
        pl.BlockSpec((rows, dloc), lambda j, c: (0, 0)),
        pl.BlockSpec((bn, dloc), lambda j, c: (off(j, c), 0)),
        pl.BlockSpec((bn, dloc), lambda j, c: (off(j, c), 0)),
        pl.BlockSpec((rows, bn), lambda j, c: (k, off(j, c))),
    ]
    args = [cvec, dy_out, dy_rem, w_own, w_oth, u_buf]
    alias = {}
    if buf is not None:
        in_specs.append(pl.BlockSpec(memory_space=pl.ANY))
        args.append(buf)
        alias = {6: 0}
    return pl.pallas_call(
        du_kernel,
        grid_spec=pltpu.PrefetchScalarGridSpec(
            num_scalar_prefetch=1, grid=(nb,), in_specs=in_specs,
            out_specs=[
                pl.BlockSpec((rows, bn), lambda j, c: (k, j)),
                pl.BlockSpec((8, bn), lambda j, c: (0, j)),
            ]),
        out_shape=[
            jax.ShapeDtypeStruct((tokens, ffh), jnp.bfloat16),
            jax.ShapeDtypeStruct((8, ffh), jnp.float32),
        ],
        input_output_aliases=alias,
        compiler_params=pltpu.CompilerParams(vmem_limit_bytes=VMEM),
        cost_estimate=pl.CostEstimate(
            flops=4 * rows * dloc * ffh, bytes_accessed=4 * (rows * dloc + dloc * ffh + rows * ffh),
            transcendentals=rows * ffh),
    )(*args)


def solution(mesh):
    swap = [(0, 1), (1, 0)]
    barrier = lax.optimization_barrier

    def swap_col(v):
        return lax.ppermute(v, 'col', swap)

    def gather_row(v):
        return lax.all_gather(v, 'row', axis=0, tiled=True)

    def local_step(x_in, ln_gain, ln_bias, w_up, b_up, w_down, b_down, dy_out):
        cid = lax.axis_index('col')
        cvec = jnp.full((1,), cid, jnp.int32)
        first = cid == 0
        tokens, dloc = x_in.shape
        width = dloc * mesh.shape['col']
        ffh = w_up.shape[1]
        xrows = tokens // NX
        yrows = tokens // NDY

        pieces = [x_in[k * xrows:(k + 1) * xrows] for k in range(NX)]
        pieces += [dy_out[k * yrows:(k + 1) * yrows] for k in range(NDY)]
        pieces = barrier(pieces)
        vecs = jnp.concatenate([ln_gain, ln_bias, b_up.astype(jnp.float32)])
        vecs_o = swap_col(vecs)
        w_up_sw = swap_col(w_up)
        x_o = [swap_col(v) for v in pieces[:NX]]
        w_dn_sw = swap_col(w_down)
        dy_o = [swap_col(v) for v in pieces[NX:]]
        w1_own = gather_row(w_up)
        w1_oth = gather_row(w_up_sw)
        w2_own = gather_row(w_down)
        db_loc = barrier(sum(jnp.sum(v.astype(jnp.float32), axis=0) for v in pieces[NX:]))

        def true_cols(own, oth):
            return jnp.concatenate([jnp.where(first, own, oth), jnp.where(first, oth, own)], axis=-1)[None]

        gain = true_cols(vecs[:dloc], vecs_o[:dloc])
        bias = true_cols(vecs[dloc:2 * dloc], vecs_o[dloc:2 * dloc])
        w1 = (w1_own, w1_oth)
        b1 = (vecs[None, 2 * dloc:], vecs_o[None, 2 * dloc:])

        z_buf, bufs, stats = None, None, []
        for k in range(NX):
            if bufs is not None:
                x_o[k], bufs, z_buf = barrier((x_o[k], bufs, z_buf))
            z_buf, st = ln_call(cvec, x_in, x_o[k], gain, bias, k, z_buf)
            stats.append(st)
            todo = [(k, 0)] + ([(k - 1, 1)] if k else []) + ([(k, 1)] if k == NX - 1 else [])
            for piece, other in todo:
                bufs = ua_call(cvec, z_buf, w1[other], b1[other], piece, other, bufs)
        w_dn_sw, bufs = barrier((w_dn_sw, bufs))
        u_buf, a_buf = bufs
        w2_oth = gather_row(w_dn_sw)

        dw2 = dot32(a_buf, dy_out, CONTRACT_ROWS)
        w2_own, dw2 = barrier((w2_own, dw2))
        dw_down = lax.psum_scatter(dw2, 'row', scatter_dimension=0, tiled=True).astype(jnp.bfloat16)
        x_f32 = x_in.astype(jnp.float32)
        y_sum = dot32(a_buf, w2_own)
        y_out = (x_f32 + y_sum + b_down.astype(jnp.float32)).astype(jnp.bfloat16)
        dy_o[0], y_out = barrier((dy_o[0], y_out))

        def du_half(other):
            buf, sums = None, []
            for k in range(NDY):
                buf, part = du_call(cvec, dy_out, dy_o[k], w2_own, w2_oth, u_buf, k, other, buf)
                sums.append(part)
            return buf, sum(sums)

        du_own, sum_own = du_half(0)
        db_up = jnp.sum(sum_own, axis=0)
        dwu = dot32(z_buf, du_own, CONTRACT_ROWS)
        dwu, u_buf = barrier((dwu, u_buf))
        dw_up = lax.psum_scatter(dwu, 'row', scatter_dimension=0, tiled=True).astype(jnp.bfloat16)
        du_oth, _ = du_half(1)

        w1_own_r = lax.dynamic_slice_in_dim(w1_own, cid * dloc, dloc, 0)
        w1_oth_r = lax.dynamic_slice_in_dim(w1_oth, cid * dloc, dloc, 0)
        dz = dot32(du_own, w1_own_r, CONTRACT_COLS) + dot32(du_oth, w1_oth_r, CONTRACT_COLS)

        st = jnp.concatenate(stats, axis=0)
        mean_x, inv_std = st[:, 0:1], st[:, 1:2]
        x_hat = (x_f32 - mean_x) * inv_std
        value_a6 = dz * ln_gain
        row_sums = jnp.concatenate([jnp.sum(value_a6, axis=1, keepdims=True), jnp.sum(value_a6 * x_hat, axis=1, keepdims=True)], axis=1)
        row_sums = lax.psum(row_sums, 'col')
        sums = lax.psum(jnp.concatenate([db_up, db_loc, jnp.sum(dz * x_hat, axis=0), jnp.sum(dz, axis=0)]), 'row')
        mean_dxh = row_sums[:, 0:1] / width
        mean_dxh_xh = row_sums[:, 1:2] / width
        dx_in = (dy_out.astype(jnp.float32) + inv_std * (value_a6 - mean_dxh - x_hat * mean_dxh_xh)).astype(jnp.bfloat16)
        db_up, db_down, d_gain, d_bias = sums[:ffh], sums[ffh:ffh + dloc], sums[ffh + dloc:ffh + 2 * dloc], sums[ffh + 2 * dloc:]
        return (y_out, dx_in, dw_up, db_up, dw_down, db_down, d_gain, d_bias)

    blk_spec = P('row', 'col')
    vec_spec = P('col')
    return jax.shard_map(local_step, mesh=mesh, in_specs=(blk_spec, vec_spec, vec_spec, blk_spec, vec_spec, blk_spec, vec_spec, blk_spec), out_specs=(blk_spec, blk_spec, blk_spec, vec_spec, blk_spec, vec_spec, vec_spec, vec_spec), check_vma=False)
```

```python
import functools

import jax
import jax.numpy as jnp
from jax import lax
from jax.experimental import pallas as pl
from jax.experimental.pallas import tpu as pltpu
from jax.sharding import PartitionSpec as P


LN_EPS = 1e-5
GELU_K = 0.7978845608028654
GELU_A = 0.044715
CONTRACT_ROWS = (((0,), (0,)), ((), ()))
CONTRACT_COLS = (((1,), (1,)), ((), ()))
CONTRACT_MM = (((1,), (0,)), ((), ()))
XCUTS = (0, 1, 2, 4)
SUB = 256
VMEM = 58 * 1024 * 1024


def gelu_pair(u_val):
    sq = u_val * u_val
    half = 0.5 + 0.5 * jnp.tanh(u_val * (GELU_K + (GELU_K * GELU_A) * sq))
    act = u_val * half
    return act, half + (act * (1.0 - half)) * (2.0 * GELU_K + (6.0 * GELU_K * GELU_A) * sq)


def dot32(a, b, dims=CONTRACT_MM):
    return lax.dot_general(a, b, dims, preferred_element_type=jnp.float32)


def ln_kernel(c_ref, xl_ref, xr_ref, g_ref, b_ref, *refs):
    z_ref, st_ref = refs[-2:]
    width = xl_ref.shape[1]
    first = c_ref[0] == 0
    xl = xl_ref[...].astype(jnp.float32)
    xr = xr_ref[...].astype(jnp.float32)
    total = jnp.sum(xl, axis=1, keepdims=True) + jnp.sum(xr, axis=1, keepdims=True)
    square = jnp.sum(xl * xl, axis=1, keepdims=True) + jnp.sum(xr * xr, axis=1, keepdims=True)
    mean = total / (2 * width)
    inv = lax.rsqrt(square / (2 * width) - mean * mean + LN_EPS)
    hl = (xl - mean) * inv
    hr = (xr - mean) * inv
    lo = jnp.where(first, hl, hr)
    hi = jnp.where(first, hr, hl)
    z_ref[:, :width] = (lo * g_ref[:, :width] + b_ref[:, :width]).astype(z_ref.dtype)
    z_ref[:, width:] = (hi * g_ref[:, width:] + b_ref[:, width:]).astype(z_ref.dtype)
    lane = lax.broadcasted_iota(jnp.int32, st_ref.shape, 1)
    st_ref[...] = jnp.where(lane == 0, mean, inv)


def ln_call(cvec, x_in, x_rem, gain, bias, start, z_buf):
    rows, width = x_rem.shape
    tokens = x_in.shape[0]
    bm = 256
    off = start // bm
    in_specs = [
        pl.BlockSpec((bm, width), lambda i, c: (off + i, 0)),
        pl.BlockSpec((bm, width), lambda i, c: (i, 0)),
        pl.BlockSpec((1, 2 * width), lambda i, c: (0, 0)),
        pl.BlockSpec((1, 2 * width), lambda i, c: (0, 0)),
    ]
    args = [cvec, x_in, x_rem, gain, bias]
    alias = {}
    if z_buf is not None:
        in_specs.append(pl.BlockSpec(memory_space=pl.ANY))
        args.append(z_buf)
        alias = {5: 0}
    return pl.pallas_call(
        ln_kernel,
        grid_spec=pltpu.PrefetchScalarGridSpec(
            num_scalar_prefetch=1,
            grid=(rows // bm,),
            in_specs=in_specs,
            out_specs=[
                pl.BlockSpec((bm, 2 * width), lambda i, c: (off + i, 0)),
                pl.BlockSpec((bm, 128), lambda i, c: (i, 0)),
            ],
        ),
        out_shape=[
            jax.ShapeDtypeStruct((tokens, 2 * width), jnp.bfloat16),
            jax.ShapeDtypeStruct((rows, 128), jnp.float32),
        ],
        input_output_aliases=alias,
        compiler_params=pltpu.CompilerParams(vmem_limit_bytes=VMEM),
        cost_estimate=pl.CostEstimate(flops=rows * width * 400, bytes_accessed=rows * width * 8, transcendentals=0),
    )(*args)


def ua_kernel(c_ref, z_ref, w_ref, b_ref, *refs):
    g_ref, a_ref = refs[-2:]
    for i in range(z_ref.shape[0] // SUB):
        part = pl.ds(i * SUB, SUB)
        u = (dot32(z_ref[part, :], w_ref[...]) + b_ref[...]).astype(a_ref.dtype)
        act, grad = gelu_pair(u.astype(jnp.float32))
        a_ref[part, :] = act.astype(a_ref.dtype)
        g_ref[part, :] = grad


def ua_call(cvec, z_buf, w_half, b_half, start, rows, other, bufs):
    tokens, width = z_buf.shape
    ffh = w_half.shape[1]
    k = start // rows
    bn = 512
    nb = ffh // bn

    def col(j, c):
        return ((1 - c[0]) if other else c[0]) * nb + j

    in_specs = [
        pl.BlockSpec((rows, width), lambda j, c: (k, 0)),
        pl.BlockSpec((width, bn), lambda j, c: (0, j)),
        pl.BlockSpec((1, bn), lambda j, c: (0, j)),
    ]
    args = [cvec, z_buf, w_half, b_half]
    alias = {}
    if bufs is not None:
        in_specs += [pl.BlockSpec(memory_space=pl.ANY)] * 2
        args += list(bufs)
        alias = {4: 0, 5: 1}
    out = pl.BlockSpec((rows, bn), lambda j, c: (k, col(j, c)))
    return pl.pallas_call(
        ua_kernel,
        grid_spec=pltpu.PrefetchScalarGridSpec(
            num_scalar_prefetch=1, grid=(nb,), in_specs=in_specs, out_specs=[out, out]),
        out_shape=[
            jax.ShapeDtypeStruct((tokens, 2 * ffh), jnp.float32),
            jax.ShapeDtypeStruct((tokens, 2 * ffh), jnp.bfloat16),
        ],
        input_output_aliases=alias,
        compiler_params=pltpu.CompilerParams(vmem_limit_bytes=VMEM),
        cost_estimate=pl.CostEstimate(
            flops=2 * rows * width * ffh, bytes_accessed=2 * (rows * width + width * ffh + 3 * rows * ffh),
            transcendentals=rows * ffh),
    )(*args)


def du_kernel(with_sum, c_ref, yl_ref, yr_ref, wl_ref, wr_ref, g_ref, du_ref, *refs):
    total = 0.0
    for i in range(yl_ref.shape[0] // SUB):
        part = pl.ds(i * SUB, SUB)
        da = dot32(yl_ref[part, :], wl_ref[...], CONTRACT_COLS) + dot32(yr_ref[part, :], wr_ref[...], CONTRACT_COLS)
        du = (da * g_ref[part, :]).astype(du_ref.dtype)
        du_ref[part, :] = du
        if with_sum:
            total += jnp.sum(du.astype(jnp.float32).reshape(SUB // 8, 8, -1), axis=0)
    if with_sum:
        refs[0][...] = total


def du_call(cvec, dy_out, dy_rem, w_own, w_oth, g_buf, other):
    tokens, dloc = dy_out.shape
    ffh = w_own.shape[0] // 2
    rows = tokens // 2
    bn = 512
    nb = ffh // bn

    def off(j, c):
        return ((1 - c[0]) if other else c[0]) * nb + j

    in_specs = [
        pl.BlockSpec((rows, dloc), lambda i, j, c: (i, 0)),
        pl.BlockSpec((rows, dloc), lambda i, j, c: (i, 0)),
        pl.BlockSpec((bn, dloc), lambda i, j, c: (off(j, c), 0)),
        pl.BlockSpec((bn, dloc), lambda i, j, c: (off(j, c), 0)),
        pl.BlockSpec((rows, bn), lambda i, j, c: (i, off(j, c))),
    ]
    out_specs = [pl.BlockSpec((rows, bn), lambda i, j, c: (i, j))]
    out_shape = [jax.ShapeDtypeStruct((tokens, ffh), jnp.bfloat16)]
    if not other:
        out_specs.append(pl.BlockSpec((8, bn), lambda i, j, c: (i, j)))
        out_shape.append(jax.ShapeDtypeStruct((8 * (tokens // rows), ffh), jnp.float32))
    return pl.pallas_call(
        functools.partial(du_kernel, not other),
        grid_spec=pltpu.PrefetchScalarGridSpec(
            num_scalar_prefetch=1, grid=(tokens // rows, nb), in_specs=in_specs, out_specs=out_specs),
        out_shape=out_shape,
        compiler_params=pltpu.CompilerParams(vmem_limit_bytes=VMEM),
        cost_estimate=pl.CostEstimate(
            flops=4 * tokens * dloc * ffh, bytes_accessed=4 * (tokens * dloc + dloc * ffh + 2 * tokens * ffh),
            transcendentals=0),
    )(cvec, dy_out, dy_rem, w_own, w_oth, g_buf)


def solution(mesh):
    swap = [(0, 1), (1, 0)]
    core_swap = [(0, 1), (1, 0), (2, 3), (3, 2)]
    x_swap = [(0, 2), (2, 0), (1, 3), (3, 1)]
    barrier = lax.optimization_barrier

    def swap_col(v):
        return lax.ppermute(v, 'col', swap)

    def gather_row(v):
        return lax.all_gather(v, 'row', axis=0, tiled=True)

    def local_step(x_in, ln_gain, ln_bias, w_up, b_up, w_down, b_down, dy_out):
        cid = lax.axis_index('col')
        cvec = jnp.full((1,), cid, jnp.int32)
        first = cid == 0
        tokens, dloc = x_in.shape
        width = dloc * mesh.shape['col']
        ffh = w_up.shape[1]
        cuts = [c * tokens // XCUTS[-1] for c in XCUTS]
        pieces = barrier([x_in[a:b] for a, b in zip(cuts, cuts[1:])] + [dy_out])
        vecs = jnp.concatenate([ln_gain, ln_bias, b_up.astype(jnp.float32)])
        vecs_o = swap_col(vecs)
        w_up_sw = swap_col(w_up)
        x_o = [swap_col(v) for v in pieces[:-1]]
        w_dn_sw = swap_col(w_down)
        dy_o = swap_col(pieces[-1])
        w1_own = gather_row(w_up)
        w1_oth = gather_row(w_up_sw)
        w2_own = gather_row(w_down)
        db_loc = barrier(jnp.sum(pieces[-1].astype(jnp.float32), axis=0))

        def true_cols(own, oth):
            return jnp.concatenate([jnp.where(first, own, oth), jnp.where(first, oth, own)], axis=-1)[None]

        gain = true_cols(vecs[:dloc], vecs_o[:dloc])
        bias = true_cols(vecs[dloc:2 * dloc], vecs_o[dloc:2 * dloc])
        w1 = (w1_own, w1_oth)
        b1 = (vecs[None, 2 * dloc:], vecs_o[None, 2 * dloc:])

        z_buf, bufs, stats = None, None, []
        todo = (((0, 1024, 0),), ((1024, 1024, 0), (0, 2048, 1)), ((2048, 2048, 0), (2048, 2048, 1)))
        for k, calls in enumerate(todo):
            if bufs is not None:
                x_o[k], bufs, z_buf = barrier((x_o[k], bufs, z_buf))
            z_buf, st = ln_call(cvec, x_in, x_o[k], gain, bias, cuts[k], z_buf)
            stats.append(st)
            for start, rows, other in calls:
                bufs = ua_call(cvec, z_buf, w1[other], b1[other], start, rows, other, bufs)
        w_dn_sw, bufs = barrier((w_dn_sw, bufs))
        g_buf, a_buf = bufs
        w2_oth = gather_row(w_dn_sw)

        dw2 = dot32(a_buf, dy_out, CONTRACT_ROWS)
        w2_own, dw2 = barrier((w2_own, dw2))
        dw_down = lax.psum_scatter(dw2, 'row', scatter_dimension=0, tiled=True).astype(jnp.bfloat16)
        x_f32 = x_in.astype(jnp.float32)
        y_sum = dot32(a_buf, w2_own)
        y_out = (x_f32 + y_sum + b_down.astype(jnp.float32)).astype(jnp.bfloat16)
        dy_o, y_out = barrier((dy_o, y_out))

        du_own, sum_own = du_call(cvec, dy_out, dy_o, w2_own, w2_oth, g_buf, 0)
        db_up = jnp.sum(sum_own, axis=0)
        n_sc = ffh * 3 // 4
        dwu = dot32(z_buf, du_own[:, :n_sc], CONTRACT_ROWS)
        du_own, dwu = barrier((du_own, dwu))
        dw_left = lax.psum_scatter(dwu, 'row', scatter_dimension=0, tiled=True).astype(jnp.bfloat16)
        rid = lax.axis_index('row')
        xid, core = rid // 2, rid % 2
        blk = dloc * mesh.shape['col'] // mesh.shape['row']

        dwu_b = dot32(z_buf, du_own[:, n_sc:], CONTRACT_ROWS)

        def dwu_rows(xi, ci):
            return lax.dynamic_slice_in_dim(dwu_b, (2 * xi + ci) * blk, blk, 0)

        got_o = lax.ppermute(dwu_rows(1 - xid, 1 - core), 'row', core_swap)
        got_s = lax.ppermute(dwu_rows(xid, 1 - core), 'row', core_swap)
        got_x = lax.ppermute(dwu_rows(1 - xid, core) + got_o, 'row', x_swap)
        keep_x = dwu_rows(xid, core) + got_s
        dwu_b, g_buf, du_own = barrier((dwu_b, g_buf, du_own))
        du_oth = du_call(cvec, dy_out, dy_o, w2_own, w2_oth, g_buf, 1)[0]

        w1_own_r = lax.dynamic_slice_in_dim(w1_own, cid * dloc, dloc, 0)
        w1_oth_r = lax.dynamic_slice_in_dim(w1_oth, cid * dloc, dloc, 0)
        dz = dot32(du_own, w1_own_r, CONTRACT_COLS) + dot32(du_oth, w1_oth_r, CONTRACT_COLS)

        st = jnp.concatenate(stats, axis=0)
        mean_x, inv_std = st[:, 0:1], st[:, 1:2]
        x_hat = (x_f32 - mean_x) * inv_std
        value_a6 = dz * ln_gain
        row_sums = jnp.concatenate([jnp.sum(value_a6, axis=1, keepdims=True), jnp.sum(value_a6 * x_hat, axis=1, keepdims=True)], axis=1)
        row_sums = row_sums + lax.ppermute(row_sums, 'col', swap)
        sums = jnp.concatenate([db_up, db_loc, jnp.sum(dz * x_hat, axis=0), jnp.sum(dz, axis=0)])
        sums = sums + lax.ppermute(sums, 'row', core_swap)
        sums = sums + lax.ppermute(sums, 'row', x_swap)
        mean_dxh = row_sums[:, 0:1] / width
        mean_dxh_xh = row_sums[:, 1:2] / width
        dx_in = (dy_out.astype(jnp.float32) + inv_std * (value_a6 - mean_dxh - x_hat * mean_dxh_xh)).astype(jnp.bfloat16)
        dw_up = jnp.concatenate([dw_left, (keep_x + got_x).astype(jnp.bfloat16)], axis=1)
        db_up, db_down, d_gain, d_bias = sums[:ffh], sums[ffh:ffh + dloc], sums[ffh + dloc:ffh + 2 * dloc], sums[ffh + 2 * dloc:]
        return (y_out, dx_in, dw_up, db_up, dw_down, db_down, d_gain, d_bias)

    blk_spec = P('row', 'col')
    vec_spec = P('col')
    return jax.shard_map(local_step, mesh=mesh, in_specs=(blk_spec, vec_spec, vec_spec, blk_spec, vec_spec, blk_spec, vec_spec, blk_spec), out_specs=(blk_spec, blk_spec, blk_spec, vec_spec, blk_spec, vec_spec, vec_spec, vec_spec), check_vma=False)
```
